32 devices in a mesh: grp: 2 (over y), page: 16 (over z, x, core).
Axes of the slice: x: 2, y: 2, z: 4, core: 2. Of those that a mesh axis runs over, the one named last changes fastest.
Arguments:
- queries: bfloat16 [32, 4096], P('grp'), parts along dimension 0, may hold values from -64 to 64
- key_cache: bfloat16 [1024, 64, 1024], P(('grp', 'page')), parts along dimension 0, may hold values from -9 to 9
- value_cache: bfloat16 [1024, 64, 1024], P(('grp', 'page')), parts along dimension 0, may hold values from -16 to 16
- new_keys: bfloat16 [32, 1024], P('grp'), parts along dimension 0, may hold values from -16 to 16
- new_values: bfloat16 [32, 1024], P('grp'), parts along dimension 0, may hold values from -6 to 6
- chosen: int32 [16, 256], P('grp', 'page'), parts along dimension 0, may hold values from 0 to 511, as said below
Outputs:
- attended: bfloat16 [32, 4096], P('grp'), parts along dimension 0
The draws below stay inside these ranges and needn't reach their ends.
There are 2 independent parts, one for each index of `grp`. The reference program is written for one: setup_inputs(seed, part) draws one part's arguments, and reference() takes and returns one part's arrays. A program takes and returns all parts, laid end to end along the dimension named above; each array names one. Nothing has to cross between parts.
Inputs may be any that keep to these rules, and one draw needn't show every extreme that they name: `chosen`: each row names 256 different pages; at most 32 of a row's pages lie in the range of 32 pages of one device, and exactly 32 do for some device in every row.
All inputs are finite; a program needn't handle non-finite values.
Results may differ from the reference program's by a relative error of at most 0.004.
Values may be sent and summed in bfloat16 or wider, within the bound.
A program may use at most 64 MiB of HBM per device.

```python
import jax
import jax.numpy as jnp
from jax import lax

MEMORY_GROUPS = 8
G = 4
D = 128
PAGE = 64
K = 256
PPD = 32
DRAFT = 16
CAPH = 32
N_PAGE = 16


def draw_chosen(key, part):
    overall_block_tally = PPD * N_PAGE
    key_order = jax.random.fold_in(key, 11)
    lookup_extra_rating = jax.random.fold_in(key, 12)
    key_heat = jax.random.fold_in(key, 13)
    precedence_rating = jax.vmap(lambda single: jax.random.permutation(single, overall_block_tally))(jax.random.split(key_order, MEMORY_GROUPS))
    precedence_rating = precedence_rating.astype(jnp.int32).reshape(MEMORY_GROUPS, N_PAGE, PPD)
    beaten = jnp.sum((precedence_rating[:, :, None, :] > precedence_rating[:, :, :, None]).astype(jnp.int32), axis=3)
    admissible_blocks = beaten < CAPH
    extra_lift_amount = jax.random.randint(lookup_extra_rating, (MEMORY_GROUPS, N_PAGE), 0, 4).astype(jnp.int32)
    strongest_blocks = jax.random.randint(key_heat, (MEMORY_GROUPS, 1), 0, N_PAGE).astype(jnp.int32)
    shard_identifiers = jnp.arange(N_PAGE, dtype=jnp.int32)[None, :]
    extra_lift_amount = jnp.where(shard_identifiers == strongest_blocks, 5, extra_lift_amount)
    block_ordering = jnp.where(admissible_blocks, extra_lift_amount[:, :, None] * overall_block_tally + precedence_rating, -1).reshape(MEMORY_GROUPS, overall_block_tally)
    picked = lax.top_k(block_ordering, K)[1]
    return picked.astype(jnp.int32)


def draw_queries(key, part):
    base = 2.0 * jax.random.normal(jax.random.fold_in(key, 21), (DRAFT, MEMORY_GROUPS * G, D), jnp.float32)
    return jnp.clip(base, -64.0, 64.0).reshape(DRAFT, MEMORY_GROUPS * G * D).astype(jnp.bfloat16)


def draw_key_cache(key, part):
    base = jax.random.normal(jax.random.fold_in(key, 31), (PPD * N_PAGE, PAGE, MEMORY_GROUPS * D), jnp.float32)
    return jnp.clip(base, -9.0, 9.0).astype(jnp.bfloat16)


def draw_value_cache(key, part):
    offsets = 1.5 * jax.random.normal(jax.random.fold_in(key, 41), (PPD * N_PAGE, 1, MEMORY_GROUPS * D), jnp.float32)
    noise = jax.random.normal(jax.random.fold_in(key, 42), (PPD * N_PAGE, PAGE, MEMORY_GROUPS * D), jnp.float32)
    return jnp.clip(noise + offsets, -16.0, 16.0).astype(jnp.bfloat16)


def bell_draw(rng, dims, scale, limit, kind=jnp.bfloat16):
    drawn = jax.random.normal(rng, dims, jnp.float32) * scale
    return jnp.minimum(jnp.maximum(drawn, -limit), limit).astype(kind)


def setup_inputs(seed: int = 0, part: int = 0) -> dict:
    seeds = jax.random.split(jax.random.key(seed), 7)
    part_splits = jax.random.split(jax.random.fold_in(seeds[6], part), 7)
    queries = draw_queries(jax.random.fold_in(jax.random.fold_in(seeds[6], part), 71), part)
    key_cache = draw_key_cache(jax.random.fold_in(jax.random.fold_in(seeds[6], part), 71), part)
    value_cache = draw_value_cache(jax.random.fold_in(jax.random.fold_in(seeds[6], part), 71), part)
    new_keys = bell_draw(part_splits[3], (DRAFT, MEMORY_GROUPS * D), 3.0, 16.0)
    new_values = bell_draw(part_splits[4], (DRAFT, MEMORY_GROUPS * D), 1.0, 6.0)
    chosen = draw_chosen(jax.random.fold_in(jax.random.fold_in(seeds[6], part), 71), part)
    return {"queries": queries, "key_cache": key_cache, "value_cache": value_cache, "new_keys": new_keys, "new_values": new_values, "chosen": chosen}


def reference(queries, key_cache, value_cache, new_keys, new_values, chosen):
    row_count = DRAFT * G
    scaling = D ** -0.5
    query_heads = queries.reshape(DRAFT, MEMORY_GROUPS, G, D).transpose(1, 0, 2, 3).reshape(MEMORY_GROUPS, row_count, D)
    key_fresh = new_keys.reshape(DRAFT, MEMORY_GROUPS, D).transpose(1, 0, 2)
    value_fresh = new_values.reshape(DRAFT, MEMORY_GROUPS, D).transpose(1, 0, 2)
    position = jnp.arange(row_count, dtype=jnp.int32) // G
    allowed = jnp.arange(DRAFT, dtype=jnp.int32)[None, :] <= position[:, None]

    def one_head(head_id):
        query_rows = query_heads[head_id]
        key_head = lax.dynamic_slice_in_dim(key_cache, head_id * D, D, 2)
        value_head = lax.dynamic_slice_in_dim(value_cache, head_id * D, D, 2)
        page_ids = chosen[head_id]
        key_rows = jnp.take(key_head, page_ids, axis=0).reshape(K * PAGE, D)
        value_rows = jnp.take(value_head, page_ids, axis=0).reshape(K * PAGE, D)
        cached = jnp.dot(query_rows, key_rows.T, preferred_element_type=jnp.float32) * scaling
        fresh_scores = jnp.dot(query_rows, key_fresh[head_id].T, preferred_element_type=jnp.float32) * scaling
        fresh_scores = jnp.where(allowed, fresh_scores, -jnp.inf)
        highest = jnp.maximum(jnp.max(cached, axis=1), jnp.max(fresh_scores, axis=1))
        weight_cached = jnp.exp(cached - highest[:, None]).astype(jnp.bfloat16)
        weight_fresh = jnp.where(allowed, jnp.exp(fresh_scores - highest[:, None]), 0.0).astype(jnp.bfloat16)
        totals = jnp.sum(weight_cached.astype(jnp.float32), axis=1) + jnp.sum(weight_fresh.astype(jnp.float32), axis=1)
        weighted = jnp.dot(weight_cached, value_rows, preferred_element_type=jnp.float32)
        weighted = weighted + jnp.dot(weight_fresh, value_fresh[head_id], preferred_element_type=jnp.float32)
        return (weighted / totals[:, None]).astype(jnp.bfloat16)

    attended = lax.map(one_head, jnp.arange(MEMORY_GROUPS, dtype=jnp.int32))
    return attended.reshape(MEMORY_GROUPS, DRAFT, G, D).transpose(1, 0, 2, 3).reshape(DRAFT, MEMORY_GROUPS * G * D)
```

```python
import functools

import jax
import jax.numpy as jnp
from jax import lax
from jax.experimental import pallas as pl
from jax.experimental.pallas import tpu as pltpu
from jax.sharding import PartitionSpec as P

LOW = -1e30
LOG2E = 1.4426950408889634
LANES = 128
BF16 = jnp.bfloat16
F32 = jnp.float32


def dot(a, b, dims):
    return lax.dot_general(a, b, (dims, ((), ())), preferred_element_type=F32)


def kernel(
    n, owners, kv_heads, groups,
    queries, key_hbm, value_hbm, new_keys, new_values, chosen, out_ref,
    kbuf, vbuf, qbd, weights, page_high, page_sums, gbuf, gsend,
    obuf, sbuf, orecv, srecv, factors, fin, finrecv,
    load_sem, g_send, g_recv, o_send, o_recv, s_send, s_recv, f_send, f_recv,
):
    me = lax.axis_index("page")
    pages, tokens, span = key_hbm.shape
    width = span // kv_heads
    drafts = queries.shape[0]
    pairs = kv_heads // 2
    rows = drafts * groups
    heads = kv_heads * groups
    per_owner = heads // owners
    per_pair = 2 * groups
    rate = width ** (-0.5) * LOG2E
    everyone = owners == n

    def peer_of(k):
        return lax.rem(me + k, n)

    loads = []
    for j in range(pairs):
        cols = pl.ds(j * 2 * width, 2 * width)
        loads.append((
            pltpu.make_async_copy(key_hbm.at[:, :, cols], kbuf.at[j], load_sem.at[0, j]),
            pltpu.make_async_copy(value_hbm.at[:, :, cols], vbuf.at[j], load_sem.at[1, j]),
        ))
    for key_load, _ in loads:
        key_load.start()
    for _, value_load in loads:
        value_load.start()

    barrier = pltpu.get_barrier_semaphore()

    def greet(k, carry):
        pl.semaphore_signal(barrier, inc=1, device_id={"page": peer_of(k)},
                            device_id_type=pl.DeviceIdType.MESH)
        return carry

    lax.fori_loop(1, n, greet, 0)

    per = chosen.shape[1]
    slots = LANES // per
    lane_ids = lax.broadcasted_iota(jnp.int32, (kv_heads, LANES), 1)
    tiled = jnp.concatenate([chosen[...]] * slots, axis=1)
    mine = jnp.where(lane_ids // per == lax.rem(me, slots), tiled, -1)
    gsend[...] = mine
    gbuf[pl.ds(me, 1)] = mine[None]

    blank = jnp.zeros((rows, width), BF16)
    for j in range(pairs):
        parts = []
        for a in range(2):
            head = 2 * j + a
            stack = jnp.concatenate(
                [queries[:, (head * groups + g) * width:(head * groups + g + 1) * width]
                 for g in range(groups)], axis=0)
            parts.append(jnp.concatenate([stack, blank] if a == 0 else [blank, stack], axis=1))
        qbd[j] = jnp.concatenate(parts, axis=0)

    pl.semaphore_wait(barrier, n - 1)

    def g_copy(k, target, slot):
        return pltpu.make_async_remote_copy(
            src_ref=gsend, dst_ref=gbuf.at[slot], send_sem=g_send.at[k], recv_sem=g_recv.at[slot],
            device_id={"page": target}, device_id_type=pl.DeviceIdType.MESH)

    def g_start(k, carry):
        g_copy(k, peer_of(k), me).start()
        return carry

    lax.fori_loop(1, n, g_start, 0)

    step = 4
    for j in range(pairs):
        loads[j][0].wait()
        for p in range(0, pages, step):
            keys = kbuf[j, p:p + step].reshape(step * tokens, 2 * width)
            scores = dot(keys, qbd[j], ((1,), (1,)))
            for i in range(step):
                part = scores[i * tokens:(i + 1) * tokens]
                high = jnp.max(part, axis=0, keepdims=True)
                raised = jnp.exp2((part - high) * rate)
                page_high[j, p + i:p + i + 1] = high
                page_sums[j, p + i:p + i + 1] = jnp.sum(raised, axis=0, keepdims=True)
                weights[j, p + i] = raised.astype(BF16)

    first = me * per_owner
    lanes = lax.broadcasted_iota(jnp.int32, (drafts, 2 * rows), 1)
    keys_at = lax.broadcasted_iota(jnp.int32, (drafts, 2 * rows), 0)
    fresh = []
    for j in range(pairs):
        cols = slice(j * 2 * width, (j + 1) * 2 * width)
        scores = dot(new_keys[:, cols], qbd[j], ((1,), (1,)))
        head_of = lanes // drafts + j * per_pair
        ok = (keys_at <= lanes % drafts) & (head_of >= first) & (head_of < first + per_owner)
        high = jnp.max(jnp.where(ok, scores, LOW), axis=0, keepdims=True)
        raised = jnp.where(ok, jnp.exp2((scores - high) * rate), 0.0)
        fresh.append((high, jnp.sum(raised, axis=0, keepdims=True), raised))

    def g_wait(k, carry):
        copy = g_copy(k, peer_of(k), peer_of(k))
        copy.wait_recv()
        copy.wait_send()
        return carry

    lax.fori_loop(1, n, g_wait, 0)

    named = [jnp.max(gbuf[t * slots:(t + 1) * slots], axis=0) for t in range(n // slots)]
    page_ids = lax.broadcasted_iota(jnp.int32, (pages, LANES), 0) + me * pages
    picked = []
    for h in range(kv_heads):
        hit = named[0][h:h + 1] == page_ids
        for other in named[1:]:
            hit = hit | (other[h:h + 1] == page_ids)
        picked.append(jnp.max(jnp.where(hit, 1.0, 0.0), axis=1, keepdims=True))
    pair_lanes = lax.broadcasted_iota(jnp.int32, (pages, 2 * rows), 1)

    def o_copy(k, target, slot, owner):
        return pltpu.make_async_remote_copy(
            src_ref=obuf.at[pl.ds(owner * per_owner, per_owner)], dst_ref=orecv.at[slot],
            send_sem=o_send.at[k], recv_sem=o_recv.at[slot],
            device_id={"page": target}, device_id_type=pl.DeviceIdType.MESH)

    def s_copy(k, target, slot, owner):
        return pltpu.make_async_remote_copy(
            src_ref=sbuf.at[owner * per_owner // per_pair], dst_ref=srecv.at[slot],
            send_sem=s_send.at[k], recv_sem=s_recv.at[slot],
            device_id={"page": target}, device_id_type=pl.DeviceIdType.MESH)

    wide = 8
    for j in range(pairs):
        in_use = jnp.where(pair_lanes < rows, picked[2 * j], picked[2 * j + 1]) > 0.5
        high_fresh, sums_fresh, raised_fresh = fresh[j]
        highs = page_high[j]
        top = jnp.maximum(jnp.max(jnp.where(in_use, highs, LOW), axis=0, keepdims=True), high_fresh)
        share = jnp.where(in_use, jnp.exp2((highs - top) * rate), 0.0).astype(BF16)
        share_fresh = jnp.exp2((high_fresh - top) * rate)
        total = jnp.sum(share.astype(F32) * page_sums[j], axis=0, keepdims=True)
        total = total + share_fresh * sums_fresh
        loads[j][1].wait()
        acc = dot((raised_fresh * share_fresh).astype(BF16),
                  new_values[:, j * 2 * width:(j + 1) * 2 * width], ((0,), (0,)))
        for p in range(0, pages, wide):
            scaled = weights[j, p:p + wide] * share[p:p + wide][:, None, :]
            acc = acc + dot(scaled.reshape(wide * tokens, 2 * rows),
                            vbuf[j, p:p + wide].reshape(wide * tokens, 2 * width), ((0,), (0,)))
        sbuf[j, 0:1] = top
        sbuf[j, 1:2] = total
        for a in range(2):
            part = acc[a * rows:(a + 1) * rows, a * width:(a + 1) * width].astype(BF16)
            obuf[(2 * j + a) * groups:(2 * j + a + 1) * groups] = part.reshape(groups, drafts, width)

        owned = per_pair // per_owner
        for o in range(j * owned, (j + 1) * owned):
            @pl.when(me != o)
            def _():
                s_copy(o, o, me, o).start()
                o_copy(o, o, me, o).start()

    def f_copy(k, target, slot):
        return pltpu.make_async_remote_copy(
            src_ref=fin, dst_ref=finrecv.at[slot], send_sem=f_send.at[k], recv_sem=f_recv.at[slot],
            device_id={"page": target}, device_id_type=pl.DeviceIdType.MESH)

    def finish():
        srecv[pl.ds(me, 1)] = sbuf[pl.ds(me * per_owner // per_pair, 1)]
        orecv[pl.ds(me, 1)] = obuf[pl.ds(first, per_owner)][None]

        def s_wait(k, carry):
            s_copy(peer_of(k), peer_of(k), peer_of(k), me).wait_recv()
            return carry

        lax.fori_loop(1, n, s_wait, 0)
        highs = srecv[:, 0, :]
        top = jnp.max(highs, axis=0, keepdims=True)
        share = jnp.exp2((highs - top) * rate)
        total = jnp.sum(share * srecv[:, 1, :], axis=0, keepdims=True)
        factors[...] = jnp.transpose(share / total)
        own_rows = per_owner * drafts
        own = factors[pl.ds(pl.multiple_of(lax.rem(first, per_pair) * drafts, drafts), own_rows), :]

        def o_wait(k, carry):
            o_copy(peer_of(k), peer_of(k), peer_of(k), me).wait_recv()
            return carry

        lax.fori_loop(1, n, o_wait, 0)
        acc = jnp.zeros((own_rows, width), F32)
        for i in range(n):
            acc = acc + own[:, i:i + 1] * orecv[i].reshape(own_rows, width).astype(F32)
        done = acc.astype(BF16).reshape(per_owner, drafts, width)
        fin[...] = done
        finrecv[pl.ds(me, 1)] = done[None]

        def f_start(k, carry):
            f_copy(k, peer_of(k), me).start()
            return carry

        lax.fori_loop(1, n, f_start, 0)

    if everyone:
        finish()
    else:
        pl.when(me < owners)(finish)

    def sent(o, carry):
        @pl.when(me != o)
        def _():
            s_copy(o, o, me, o).wait_send()
            o_copy(o, o, me, o).wait_send()
        return carry

    lax.fori_loop(0, owners, sent, 0)

    def f_wait(o, carry):
        @pl.when(me != o)
        def _():
            f_copy(o, o, o).wait_recv()
        return carry

    lax.fori_loop(0, owners, f_wait, 0)
    for o in range(owners):
        for i in range(per_owner):
            head = o * per_owner + i
            out_ref[:, head * width:(head + 1) * width] = finrecv[o, i]

    def f_sent():
        def body(k, carry):
            f_copy(k, peer_of(k), me).wait_send()
            return carry

        lax.fori_loop(1, n, body, 0)

    if everyone:
        f_sent()
    else:
        pl.when(me < owners)(f_sent)


def on_device(queries, key_cache, value_cache, new_keys, new_values, chosen):
    n = lax.axis_size("page")
    pages, tokens, span = key_cache.shape
    drafts = queries.shape[0]
    groups = queries.shape[1] // span
    kv_heads = chosen.shape[0]
    width = span // kv_heads
    pairs = kv_heads // 2
    heads = kv_heads * groups
    rows = drafts * groups
    owners = min(n, heads)
    per_owner = heads // owners
    vmem = pl.BlockSpec(memory_space=pltpu.VMEM)
    hbm = pl.BlockSpec(memory_space=pl.ANY)
    dma = pltpu.SemaphoreType.DMA
    return pl.pallas_call(
        functools.partial(kernel, n, owners, kv_heads, groups),
        out_shape=jax.ShapeDtypeStruct(queries.shape, BF16),
        in_specs=[vmem, hbm, hbm, vmem, vmem, vmem],
        out_specs=vmem,
        scratch_shapes=[
            pltpu.VMEM((pairs, pages, tokens, 2 * width), BF16),
            pltpu.VMEM((pairs, pages, tokens, 2 * width), BF16),
            pltpu.VMEM((pairs, 2 * rows, 2 * width), BF16),
            pltpu.VMEM((pairs, pages, tokens, 2 * rows), BF16),
            pltpu.VMEM((pairs, pages, 2 * rows), F32),
            pltpu.VMEM((pairs, pages, 2 * rows), F32),
            pltpu.VMEM((n, kv_heads, LANES), jnp.int32),
            pltpu.VMEM((kv_heads, LANES), jnp.int32),
            pltpu.VMEM((heads, drafts, width), BF16),
            pltpu.VMEM((pairs, 2, 2 * rows), F32),
            pltpu.VMEM((n, per_owner, drafts, width), BF16),
            pltpu.VMEM((n, 2, 2 * rows), F32),
            pltpu.VMEM((2 * rows, n), F32),
            pltpu.VMEM((per_owner, drafts, width), BF16),
            pltpu.VMEM((owners, per_owner, drafts, width), BF16),
            dma((2, pairs)),
            dma((n,)), dma((n,)),
            dma((n,)), dma((n,)),
            dma((n,)), dma((n,)),
            dma((n,)), dma((n,)),
        ],
        compiler_params=pltpu.CompilerParams(collective_id=0, has_side_effects=True),
        name="paged_attention",
    )(queries, key_cache, value_cache, new_keys, new_values, chosen)


def solution(mesh):
    placed = (
        P("grp", None),
        P(("grp", "page"), None, None),
        P(("grp", "page"), None, None),
        P("grp", None),
        P("grp", None),
        P("grp", "page"),
    )
    return jax.shard_map(
        on_device, mesh=mesh, in_specs=placed, out_specs=P("grp", None), check_vma=False
    )
```

```python
import functools

import jax
import jax.numpy as jnp
from jax import lax
from jax.experimental import pallas as pl
from jax.experimental.pallas import tpu as pltpu
from jax.sharding import PartitionSpec as P

LOW = -1e30
LOG2E = 1.4426950408889634
LANES = 128
BF16 = jnp.bfloat16
F32 = jnp.float32


def dot(a, b, dims):
    return lax.dot_general(a, b, (dims, ((), ())), preferred_element_type=F32)


def kernel(
    n, owners, kv_heads, groups,
    queries_hbm, key_hbm, value_hbm, new_keys_hbm, new_values_hbm, chosen_hbm, out_ref,
    queries, new_keys, new_values, chosen, kbuf, vbuf, qbd, weights, page_high, page_sums, gbuf, gsend,
    obuf, sbuf, orecv, srecv, factors, fin,
    small_sem, load_sem, g_send, g_recv, o_send, o_recv, s_send, s_recv, f_send, f_recv,
):
    me = lax.axis_index("page")
    pages, tokens, span = key_hbm.shape
    width = span // kv_heads
    drafts = queries.shape[0]
    pairs = kv_heads // 2
    rows = drafts * groups
    heads = kv_heads * groups
    per_owner = heads // owners
    per_pair = 2 * groups
    rate = width ** (-0.5) * LOG2E
    everyone = owners == n

    def peer_of(k):
        return lax.rem(me + k, n)

    barrier = pltpu.get_barrier_semaphore()

    def greet(k, carry):
        pl.semaphore_signal(barrier, inc=1, device_id={"page": peer_of(k)},
                            device_id_type=pl.DeviceIdType.MESH)
        return carry

    lax.fori_loop(1, n, greet, 0)

    small = [
        pltpu.make_async_copy(src, dst, small_sem.at[i])
        for i, (src, dst) in enumerate((
            (chosen_hbm, chosen), (queries_hbm, queries),
            (new_keys_hbm, new_keys), (new_values_hbm, new_values)))
    ]
    small[0].start()
    small[1].start()
    loads = []
    for j in range(pairs):
        cols = pl.ds(j * 2 * width, 2 * width)
        loads.append((
            pltpu.make_async_copy(key_hbm.at[:, :, cols], kbuf.at[j], load_sem.at[0, j]),
            pltpu.make_async_copy(value_hbm.at[:, :, cols], vbuf.at[j], load_sem.at[1, j]),
        ))
    for key_load, _ in loads:
        key_load.start()
    for _, value_load in loads:
        value_load.start()
    small[2].start()
    small[3].start()

    per = chosen.shape[1]
    slots = LANES // per
    lane_ids = lax.broadcasted_iota(jnp.int32, (kv_heads, LANES), 1)
    small[0].wait()
    tiled = jnp.concatenate([chosen[...]] * slots, axis=1)
    mine = jnp.where(lane_ids // per == lax.rem(me, slots), tiled, -1)
    gsend[...] = mine
    gbuf[pl.ds(me, 1)] = mine[None]

    pl.semaphore_wait(barrier, n - 1)

    def g_copy(k, target, slot):
        return pltpu.make_async_remote_copy(
            src_ref=gsend, dst_ref=gbuf.at[slot], send_sem=g_send.at[k], recv_sem=g_recv.at[slot],
            device_id={"page": target}, device_id_type=pl.DeviceIdType.MESH)

    def g_start(k, carry):
        g_copy(k, peer_of(k), me).start()
        return carry

    lax.fori_loop(1, n, g_start, 0)

    small[1].wait()
    blank = jnp.zeros((rows, width), BF16)
    for j in range(pairs):
        parts = []
        for a in range(2):
            head = 2 * j + a
            stack = jnp.concatenate(
                [queries[:, (head * groups + g) * width:(head * groups + g + 1) * width]
                 for g in range(groups)], axis=0)
            parts.append(jnp.concatenate([stack, blank] if a == 0 else [blank, stack], axis=1))
        qbd[j] = jnp.concatenate(parts, axis=0)

    step = 4
    for j in range(pairs):
        loads[j][0].wait()
        for p in range(0, pages, step):
            keys = kbuf[j, p:p + step].reshape(step * tokens, 2 * width)
            scores = dot(keys, qbd[j], ((1,), (1,)))
            for i in range(step):
                part = scores[i * tokens:(i + 1) * tokens]
                high = jnp.ceil(jnp.max(part, axis=0, keepdims=True) * rate)
                raised = jnp.exp2(part * rate - high)
                page_high[j, p + i:p + i + 1] = high
                page_sums[j, p + i:p + i + 1] = jnp.sum(raised, axis=0, keepdims=True)
                weights[j, p + i] = raised.astype(BF16)

    first = me * per_owner
    lanes = lax.broadcasted_iota(jnp.int32, (drafts, 2 * rows), 1)
    keys_at = lax.broadcasted_iota(jnp.int32, (drafts, 2 * rows), 0)
    fresh = []
    small[2].wait()
    small[3].wait()
    for j in range(pairs):
        cols = slice(j * 2 * width, (j + 1) * 2 * width)
        scores = dot(new_keys[:, cols], qbd[j], ((1,), (1,)))
        head_of = lanes // drafts + j * per_pair
        ok = (keys_at <= lanes % drafts) & (head_of >= first) & (head_of < first + per_owner)
        high = jnp.ceil(jnp.max(jnp.where(ok, scores * rate, LOW), axis=0, keepdims=True))
        raised = jnp.where(ok, jnp.exp2(scores * rate - high), 0.0)
        fresh.append((high, jnp.sum(raised, axis=0, keepdims=True), raised))

    def g_wait(k, carry):
        copy = g_copy(k, peer_of(k), peer_of(k))
        copy.wait_recv()
        copy.wait_send()
        return carry

    lax.fori_loop(1, n, g_wait, 0)

    named = [jnp.max(gbuf[t * slots:(t + 1) * slots], axis=0) for t in range(n // slots)]
    page_ids = lax.broadcasted_iota(jnp.int32, (pages, LANES), 0) + me * pages
    picked = []
    for h in range(kv_heads):
        hit = named[0][h:h + 1] == page_ids
        for other in named[1:]:
            hit = hit | (other[h:h + 1] == page_ids)
        picked.append(jnp.max(jnp.where(hit, 1.0, 0.0), axis=1, keepdims=True))
    pair_lanes = lax.broadcasted_iota(jnp.int32, (pages, 2 * rows), 1)

    def o_copy(k, target, slot, owner):
        return pltpu.make_async_remote_copy(
            src_ref=obuf.at[pl.ds(owner * per_owner, per_owner)], dst_ref=orecv.at[slot],
            send_sem=o_send.at[k], recv_sem=o_recv.at[slot],
            device_id={"page": target}, device_id_type=pl.DeviceIdType.MESH)

    def s_copy(k, target, slot, owner):
        return pltpu.make_async_remote_copy(
            src_ref=sbuf.at[owner * per_owner // per_pair], dst_ref=srecv.at[slot],
            send_sem=s_send.at[k], recv_sem=s_recv.at[slot],
            device_id={"page": target}, device_id_type=pl.DeviceIdType.MESH)

    wide = 8
    for j in range(pairs):
        in_use = jnp.where(pair_lanes < rows, picked[2 * j], picked[2 * j + 1]) > 0.5
        high_fresh, sums_fresh, raised_fresh = fresh[j]
        highs = page_high[j]
        top = jnp.maximum(jnp.max(jnp.where(in_use, highs, LOW), axis=0, keepdims=True), high_fresh)
        share = jnp.where(in_use, jnp.exp2(highs - top), 0.0).astype(BF16)
        share_fresh = jnp.exp2(high_fresh - top)
        total = jnp.sum(share.astype(F32) * page_sums[j], axis=0, keepdims=True)
        total = total + share_fresh * sums_fresh
        loads[j][1].wait()
        acc = dot((raised_fresh * share_fresh).astype(BF16),
                  new_values[:, j * 2 * width:(j + 1) * 2 * width], ((0,), (0,)))
        for p in range(0, pages, wide):
            scaled = weights[j, p:p + wide] * share[p:p + wide][:, None, :]
            acc = acc + dot(scaled.reshape(wide * tokens, 2 * rows),
                            vbuf[j, p:p + wide].reshape(wide * tokens, 2 * width), ((0,), (0,)))
        sbuf[j, 0:1] = top
        sbuf[j, 1:2] = total
        for a in range(2):
            part = acc[a * rows:(a + 1) * rows, a * width:(a + 1) * width].astype(BF16)
            obuf[(2 * j + a) * groups:(2 * j + a + 1) * groups] = part.reshape(groups, drafts, width)

        owned = per_pair // per_owner
        for o in range(j * owned, (j + 1) * owned):
            @pl.when(me != o)
            def _():
                s_copy(o, o, me, o).start()
                o_copy(o, o, me, o).start()

    def block_of(owner):
        cols = per_owner * width
        return out_ref.at[:, pl.ds(pl.multiple_of(owner * cols, cols), cols)]

    def f_copy(k, target, slot):
        return pltpu.make_async_remote_copy(
            src_ref=fin, dst_ref=block_of(slot), send_sem=f_send.at[k], recv_sem=f_recv.at[slot],
            device_id={"page": target}, device_id_type=pl.DeviceIdType.MESH)

    def finish():
        srecv[pl.ds(me, 1)] = sbuf[pl.ds(me * per_owner // per_pair, 1)]
        orecv[pl.ds(me, 1)] = obuf[pl.ds(first, per_owner)][None]

        def s_wait(k, carry):
            s_copy(peer_of(k), peer_of(k), peer_of(k), me).wait_recv()
            return carry

        lax.fori_loop(1, n, s_wait, 0)
        highs = srecv[:, 0, :]
        top = jnp.max(highs, axis=0, keepdims=True)
        share = jnp.exp2(highs - top)
        total = jnp.sum(share * srecv[:, 1, :], axis=0, keepdims=True)
        factors[...] = jnp.transpose(share / total)
        own_rows = per_owner * drafts
        own = factors[pl.ds(pl.multiple_of(lax.rem(first, per_pair) * drafts, drafts), own_rows), :]

        def o_wait(k, carry):
            o_copy(peer_of(k), peer_of(k), peer_of(k), me).wait_recv()
            return carry

        lax.fori_loop(1, n, o_wait, 0)
        acc = jnp.zeros((own_rows, width), F32)
        for i in range(n):
            acc = acc + own[:, i:i + 1] * orecv[i].reshape(own_rows, width).astype(F32)
        done = acc.astype(BF16)
        for i in range(per_owner):
            fin[:, i * width:(i + 1) * width] = done[i * drafts:(i + 1) * drafts]

        def f_start(k, carry):
            f_copy(k, peer_of(k), me).start()
            return carry

        lax.fori_loop(1, n, f_start, 0)
        block_of(me)[...] = fin[...]

    if everyone:
        finish()
    else:
        pl.when(me < owners)(finish)

    def sent(o, carry):
        @pl.when(me != o)
        def _():
            s_copy(o, o, me, o).wait_send()
            o_copy(o, o, me, o).wait_send()
        return carry

    lax.fori_loop(0, owners, sent, 0)

    def f_wait(o, carry):
        @pl.when(me != o)
        def _():
            f_copy(o, o, o).wait_recv()
        return carry

    lax.fori_loop(0, owners, f_wait, 0)
    def f_sent():
        def body(k, carry):
            f_copy(k, peer_of(k), me).wait_send()
            return carry

        lax.fori_loop(1, n, body, 0)

    if everyone:
        f_sent()
    else:
        pl.when(me < owners)(f_sent)


def on_device(queries, key_cache, value_cache, new_keys, new_values, chosen):
    n = lax.axis_size("page")
    pages, tokens, span = key_cache.shape
    drafts = queries.shape[0]
    groups = queries.shape[1] // span
    kv_heads = chosen.shape[0]
    width = span // kv_heads
    pairs = kv_heads // 2
    heads = kv_heads * groups
    rows = drafts * groups
    owners = min(n, heads)
    per_owner = heads // owners
    vmem = pl.BlockSpec(memory_space=pltpu.VMEM)
    hbm = pl.BlockSpec(memory_space=pl.ANY)
    dma = pltpu.SemaphoreType.DMA
    return pl.pallas_call(
        functools.partial(kernel, n, owners, kv_heads, groups),
        out_shape=pltpu.VMEM(queries.shape, BF16),
        in_specs=[hbm] * 6,
        out_specs=vmem,
        scratch_shapes=[
            pltpu.VMEM(queries.shape, BF16),
            pltpu.VMEM(new_keys.shape, BF16),
            pltpu.VMEM(new_values.shape, BF16),
            pltpu.VMEM(chosen.shape, jnp.int32),
            pltpu.VMEM((pairs, pages, tokens, 2 * width), BF16),
            pltpu.VMEM((pairs, pages, tokens, 2 * width), BF16),
            pltpu.VMEM((pairs, 2 * rows, 2 * width), BF16),
            pltpu.VMEM((pairs, pages, tokens, 2 * rows), BF16),
            pltpu.VMEM((pairs, pages, 2 * rows), F32),
            pltpu.VMEM((pairs, pages, 2 * rows), F32),
            pltpu.VMEM((n, kv_heads, LANES), jnp.int32),
            pltpu.VMEM((kv_heads, LANES), jnp.int32),
            pltpu.VMEM((heads, drafts, width), BF16),
            pltpu.VMEM((pairs, 2, 2 * rows), F32),
            pltpu.VMEM((n, per_owner, drafts, width), BF16),
            pltpu.VMEM((n, 2, 2 * rows), F32),
            pltpu.VMEM((2 * rows, n), F32),
            pltpu.VMEM((drafts, per_owner * width), BF16),
            dma((4,)), dma((2, pairs)),
            dma((n,)), dma((n,)),
            dma((n,)), dma((n,)),
            dma((n,)), dma((n,)),
            dma((n,)), dma((n,)),
        ],
        compiler_params=pltpu.CompilerParams(collective_id=0, has_side_effects=True),
        name="paged_attention",
    )(queries, key_cache, value_cache, new_keys, new_values, chosen)


def solution(mesh):
    placed = (
        P("grp", None),
        P(("grp", "page"), None, None),
        P(("grp", "page"), None, None),
        P("grp", None),
        P("grp", None),
        P("grp", "page"),
    )
    return jax.shard_map(
        on_device, mesh=mesh, in_specs=placed, out_specs=P("grp", None), check_vma=False
    )
```

```python
import functools

import jax
import jax.numpy as jnp
from jax import lax
from jax.experimental import pallas as pl
from jax.experimental.pallas import tpu as pltpu
from jax.sharding import PartitionSpec as P

LOW = -1e30
LOG2E = 1.4426950408889634
LANES = 128
BF16 = jnp.bfloat16
F32 = jnp.float32


def dot(a, b, dims):
    return lax.dot_general(a, b, (dims, ((), ())), preferred_element_type=F32)


def kernel(
    n, owners, kv_heads, groups,
    queries_hbm, key_hbm, value_hbm, new_keys_hbm, new_values_hbm, chosen_hbm, out_ref,
    queries, new_keys, new_values, chosen, kbuf, vbuf, qbd, weights, page_high, page_sums, gbuf, gsend,
    obuf, sbuf, orecv, srecv, factors, fin,
    small_sem, load_sem, g_send, g_recv, o_send, o_recv, s_send, s_recv, f_send, f_recv,
):
    me = lax.axis_index("page")
    pages, tokens, span = key_hbm.shape
    width = span // kv_heads
    drafts = queries.shape[0]
    pairs = kv_heads // 2
    rows = drafts * groups
    heads = kv_heads * groups
    per_owner = heads // owners
    per_pair = 2 * groups
    rate = width ** (-0.5) * LOG2E
    everyone = owners == n

    def peer_of(k):
        return lax.rem(me + k, n)

    barrier = pltpu.get_barrier_semaphore()

    def greet(k, carry):
        pl.semaphore_signal(barrier, inc=1, device_id={"page": peer_of(k)},
                            device_id_type=pl.DeviceIdType.MESH)
        return carry

    lax.fori_loop(1, n, greet, 0)

    small = [
        pltpu.make_async_copy(src, dst, small_sem.at[i])
        for i, (src, dst) in enumerate((
            (chosen_hbm, chosen), (queries_hbm, queries),
            (new_keys_hbm, new_keys), (new_values_hbm, new_values)))
    ]
    small[0].start()
    small[1].start()
    loads = []
    for j in range(pairs):
        cols = pl.ds(j * 2 * width, 2 * width)
        loads.append((
            pltpu.make_async_copy(key_hbm.at[:, :, cols], kbuf.at[j], load_sem.at[0, j]),
            pltpu.make_async_copy(value_hbm.at[:, :, cols], vbuf.at[j], load_sem.at[1, j]),
        ))
    for key_load, _ in loads:
        key_load.start()
    for _, value_load in loads:
        value_load.start()
    small[2].start()
    small[3].start()

    per = chosen.shape[1]
    slots = LANES // per
    lane_ids = lax.broadcasted_iota(jnp.int32, (kv_heads, LANES), 1)
    small[0].wait()
    tiled = jnp.concatenate([chosen[...]] * slots, axis=1)
    mine = jnp.where(lane_ids // per == lax.rem(me, slots), tiled, -1)
    gsend[...] = mine
    gbuf[pl.ds(me, 1)] = mine[None]

    pl.semaphore_wait(barrier, n - 1)

    def g_copy(k, target, slot):
        return pltpu.make_async_remote_copy(
            src_ref=gsend, dst_ref=gbuf.at[slot], send_sem=g_send.at[k], recv_sem=g_recv.at[slot],
            device_id={"page": target}, device_id_type=pl.DeviceIdType.MESH)

    def g_start(k, carry):
        g_copy(k, peer_of(k), me).start()
        return carry

    lax.fori_loop(1, n, g_start, 0)

    small[1].wait()
    blank = jnp.zeros((rows, width), BF16)
    for j in range(pairs):
        parts = []
        for a in range(2):
            head = 2 * j + a
            stack = jnp.concatenate(
                [queries[:, (head * groups + g) * width:(head * groups + g + 1) * width]
                 for g in range(groups)], axis=0)
            parts.append(jnp.concatenate([stack, blank] if a == 0 else [blank, stack], axis=1))
        qbd[j] = jnp.concatenate(parts, axis=0)

    step = 4
    for j in range(pairs):
        loads[j][0].wait()
        for p in range(0, pages, step):
            keys = kbuf[j, p:p + step].reshape(step * tokens, 2 * width)
            scores = dot(keys, qbd[j], ((1,), (1,)))
            for i in range(step):
                part = scores[i * tokens:(i + 1) * tokens]
                high = jnp.ceil(jnp.max(part, axis=0, keepdims=True) * rate)
                raised = jnp.exp2(part * rate - high).astype(BF16)
                page_high[j, p + i:p + i + 1] = high
                page_sums[j, p + i:p + i + 1] = jnp.sum(raised.astype(F32), axis=0, keepdims=True)
                weights[j, p + i] = raised

    first = me * per_owner
    lanes = lax.broadcasted_iota(jnp.int32, (drafts, 2 * rows), 1)
    keys_at = lax.broadcasted_iota(jnp.int32, (drafts, 2 * rows), 0)
    fresh = []
    small[2].wait()
    small[3].wait()
    for j in range(pairs):
        cols = slice(j * 2 * width, (j + 1) * 2 * width)
        scores = dot(new_keys[:, cols], qbd[j], ((1,), (1,)))
        head_of = lanes // drafts + j * per_pair
        ok = (keys_at <= lanes % drafts) & (head_of >= first) & (head_of < first + per_owner)
        high = jnp.ceil(jnp.max(jnp.where(ok, scores * rate, LOW), axis=0, keepdims=True))
        raised = jnp.where(ok, jnp.exp2(scores * rate - high), 0.0).astype(BF16).astype(F32)
        fresh.append((high, jnp.sum(raised, axis=0, keepdims=True), raised))

    def g_wait(k, carry):
        copy = g_copy(k, peer_of(k), peer_of(k))
        copy.wait_recv()
        copy.wait_send()
        return carry

    lax.fori_loop(1, n, g_wait, 0)

    named = [jnp.max(gbuf[t * slots:(t + 1) * slots], axis=0) for t in range(n // slots)]
    page_ids = lax.broadcasted_iota(jnp.int32, (pages, LANES), 0) + me * pages
    picked = []
    for h in range(kv_heads):
        hit = named[0][h:h + 1] == page_ids
        for other in named[1:]:
            hit = hit | (other[h:h + 1] == page_ids)
        picked.append(jnp.max(jnp.where(hit, 1.0, 0.0), axis=1, keepdims=True))
    pair_lanes = lax.broadcasted_iota(jnp.int32, (pages, 2 * rows), 1)

    def o_copy(k, target, slot, owner):
        return pltpu.make_async_remote_copy(
            src_ref=obuf.at[pl.ds(owner * per_owner, per_owner)], dst_ref=orecv.at[slot],
            send_sem=o_send.at[k], recv_sem=o_recv.at[slot],
            device_id={"page": target}, device_id_type=pl.DeviceIdType.MESH)

    def s_copy(k, target, slot, owner):
        return pltpu.make_async_remote_copy(
            src_ref=sbuf.at[owner * per_owner // per_pair], dst_ref=srecv.at[slot],
            send_sem=s_send.at[k], recv_sem=s_recv.at[slot],
            device_id={"page": target}, device_id_type=pl.DeviceIdType.MESH)

    wide = 8
    for j in range(pairs):
        in_use = jnp.where(pair_lanes < rows, picked[2 * j], picked[2 * j + 1]) > 0.5
        high_fresh, sums_fresh, raised_fresh = fresh[j]
        highs = page_high[j]
        top = jnp.maximum(jnp.max(jnp.where(in_use, highs, LOW), axis=0, keepdims=True), high_fresh)
        share = jnp.where(in_use, jnp.exp2(highs - top), 0.0).astype(BF16)
        share_fresh = jnp.exp2(high_fresh - top)
        total = jnp.sum(share.astype(F32) * page_sums[j], axis=0, keepdims=True)
        total = total + share_fresh * sums_fresh
        loads[j][1].wait()
        acc = dot((raised_fresh * share_fresh).astype(BF16),
                  new_values[:, j * 2 * width:(j + 1) * 2 * width], ((0,), (0,)))
        for p in range(0, pages, wide):
            scaled = weights[j, p:p + wide] * share[p:p + wide][:, None, :]
            acc = acc + dot(scaled.reshape(wide * tokens, 2 * rows),
                            vbuf[j, p:p + wide].reshape(wide * tokens, 2 * width), ((0,), (0,)))
        sbuf[j, 0:1] = top
        sbuf[j, 1:2] = total
        for a in range(2):
            part = acc[a * rows:(a + 1) * rows, a * width:(a + 1) * width].astype(BF16)
            obuf[(2 * j + a) * groups:(2 * j + a + 1) * groups] = part.reshape(groups, drafts, width)

        owned = per_pair // per_owner
        for o in range(j * owned, (j + 1) * owned):
            @pl.when(me != o)
            def _():
                s_copy(o, o, me, o).start()
                o_copy(o, o, me, o).start()

    def block_of(owner):
        cols = per_owner * width
        return out_ref.at[:, pl.ds(pl.multiple_of(owner * cols, cols), cols)]

    def f_copy(k, target, slot):
        return pltpu.make_async_remote_copy(
            src_ref=fin, dst_ref=block_of(slot), send_sem=f_send.at[k], recv_sem=f_recv.at[slot],
            device_id={"page": target}, device_id_type=pl.DeviceIdType.MESH)

    def finish():
        srecv[pl.ds(me, 1)] = sbuf[pl.ds(me * per_owner // per_pair, 1)]
        orecv[pl.ds(me, 1)] = obuf[pl.ds(first, per_owner)][None]

        def s_wait(k, carry):
            s_copy(peer_of(k), peer_of(k), peer_of(k), me).wait_recv()
            return carry

        lax.fori_loop(1, n, s_wait, 0)
        highs = srecv[:, 0, :]
        top = jnp.max(highs, axis=0, keepdims=True)
        share = jnp.exp2(highs - top)
        total = jnp.sum(share * srecv[:, 1, :], axis=0, keepdims=True)
        factors[...] = jnp.transpose(share / total)
        own_rows = per_owner * drafts
        own = factors[pl.ds(pl.multiple_of(lax.rem(first, per_pair) * drafts, drafts), own_rows), :]

        def o_wait(k, carry):
            o_copy(peer_of(k), peer_of(k), peer_of(k), me).wait_recv()
            return carry

        lax.fori_loop(1, n, o_wait, 0)
        acc = jnp.zeros((own_rows, width), F32)
        for i in range(n):
            acc = acc + own[:, i:i + 1] * orecv[i].reshape(own_rows, width).astype(F32)
        done = acc.astype(BF16)
        for i in range(per_owner):
            fin[:, i * width:(i + 1) * width] = done[i * drafts:(i + 1) * drafts]

        def f_start(k, carry):
            f_copy(k, peer_of(k), me).start()
            return carry

        lax.fori_loop(1, n, f_start, 0)
        block_of(me)[...] = fin[...]

    if everyone:
        finish()
    else:
        pl.when(me < owners)(finish)

    def sent(o, carry):
        @pl.when(me != o)
        def _():
            s_copy(o, o, me, o).wait_send()
            o_copy(o, o, me, o).wait_send()
        return carry

    lax.fori_loop(0, owners, sent, 0)

    def f_wait(o, carry):
        @pl.when(me != o)
        def _():
            f_copy(o, o, o).wait_recv()
        return carry

    lax.fori_loop(0, owners, f_wait, 0)
    def f_sent():
        def body(k, carry):
            f_copy(k, peer_of(k), me).wait_send()
            return carry

        lax.fori_loop(1, n, body, 0)

    if everyone:
        f_sent()
    else:
        pl.when(me < owners)(f_sent)


def on_device(queries, key_cache, value_cache, new_keys, new_values, chosen):
    n = lax.axis_size("page")
    pages, tokens, span = key_cache.shape
    drafts = queries.shape[0]
    groups = queries.shape[1] // span
    kv_heads = chosen.shape[0]
    width = span // kv_heads
    pairs = kv_heads // 2
    heads = kv_heads * groups
    rows = drafts * groups
    owners = min(n, heads)
    per_owner = heads // owners
    vmem = pl.BlockSpec(memory_space=pltpu.VMEM)
    hbm = pl.BlockSpec(memory_space=pl.ANY)
    dma = pltpu.SemaphoreType.DMA
    return pl.pallas_call(
        functools.partial(kernel, n, owners, kv_heads, groups),
        out_shape=pltpu.VMEM(queries.shape, BF16),
        in_specs=[hbm] * 6,
        out_specs=vmem,
        scratch_shapes=[
            pltpu.VMEM(queries.shape, BF16),
            pltpu.VMEM(new_keys.shape, BF16),
            pltpu.VMEM(new_values.shape, BF16),
            pltpu.VMEM(chosen.shape, jnp.int32),
            pltpu.VMEM((pairs, pages, tokens, 2 * width), BF16),
            pltpu.VMEM((pairs, pages, tokens, 2 * width), BF16),
            pltpu.VMEM((pairs, 2 * rows, 2 * width), BF16),
            pltpu.VMEM((pairs, pages, tokens, 2 * rows), BF16),
            pltpu.VMEM((pairs, pages, 2 * rows), F32),
            pltpu.VMEM((pairs, pages, 2 * rows), F32),
            pltpu.VMEM((n, kv_heads, LANES), jnp.int32),
            pltpu.VMEM((kv_heads, LANES), jnp.int32),
            pltpu.VMEM((heads, drafts, width), BF16),
            pltpu.VMEM((pairs, 2, 2 * rows), F32),
            pltpu.VMEM((n, per_owner, drafts, width), BF16),
            pltpu.VMEM((n, 2, 2 * rows), F32),
            pltpu.VMEM((2 * rows, n), F32),
            pltpu.VMEM((drafts, per_owner * width), BF16),
            dma((4,)), dma((2, pairs)),
            dma((n,)), dma((n,)),
            dma((n,)), dma((n,)),
            dma((n,)), dma((n,)),
            dma((n,)), dma((n,)),
        ],
        compiler_params=pltpu.CompilerParams(collective_id=0, has_side_effects=True),
        name="paged_attention",
    )(queries, key_cache, value_cache, new_keys, new_values, chosen)


def solution(mesh):
    placed = (
        P("grp", None),
        P(("grp", "page"), None, None),
        P(("grp", "page"), None, None),
        P("grp", None),
        P("grp", None),
        P("grp", "page"),
    )
    return jax.shard_map(
        on_device, mesh=mesh, in_specs=placed, out_specs=P("grp", None), check_vma=False
    )
```

```python
import functools

import jax
import jax.numpy as jnp
from jax import lax
from jax.experimental import pallas as pl
from jax.experimental.pallas import tpu as pltpu
from jax.sharding import PartitionSpec as P

LOW = -1e30
LOG2E = 1.4426950408889634
LANES = 128
BF16 = jnp.bfloat16
F32 = jnp.float32


def dot(a, b, dims):
    return lax.dot_general(a, b, (dims, ((), ())), preferred_element_type=F32)


def kernel(
    n, owners, kv_heads, groups,
    queries_hbm, key_hbm, value_hbm, new_keys_hbm, new_values_hbm, chosen_hbm, out_ref,
    queries, new_keys, new_values, chosen, kbuf, vbuf, qbd, weights, page_high, page_sums, gbuf, gsend, picked, fresh_stats, fresh_weights,
    obuf, sbuf, orecv, srecv, factors, fin,
    small_sem, load_sem, g_send, g_recv, o_send, o_recv, s_send, s_recv, f_send, f_recv,
):
    me = lax.axis_index("page")
    pages, tokens, span = key_hbm.shape
    width = span // kv_heads
    drafts = queries.shape[0]
    pairs = kv_heads // 2
    rows = drafts * groups
    heads = kv_heads * groups
    per_owner = heads // owners
    per_pair = 2 * groups
    rate = width ** (-0.5) * LOG2E
    everyone = owners == n

    def peer_of(k):
        return lax.rem(me + k, n)

    def far_first(count, act):
        def body(k, carry):
            peer = jnp.where(me * 2 < n, count - 1 - k, k)
            pl.when(peer != me)(lambda: act(peer))
            return carry

        lax.fori_loop(0, count, body, 0)

    barrier = pltpu.get_barrier_semaphore()

    def greet(k, carry):
        pl.semaphore_signal(barrier, inc=1, device_id={"page": peer_of(k)},
                            device_id_type=pl.DeviceIdType.MESH)
        return carry

    lax.fori_loop(1, n, greet, 0)

    small = [
        pltpu.make_async_copy(src, dst, small_sem.at[i])
        for i, (src, dst) in enumerate((
            (chosen_hbm, chosen), (queries_hbm, queries),
            (new_keys_hbm, new_keys), (new_values_hbm, new_values)))
    ]
    small[0].start()
    small[1].start()
    loads = []
    for j in range(pairs):
        cols = pl.ds(j * 2 * width, 2 * width)
        loads.append((
            pltpu.make_async_copy(key_hbm.at[:, :, cols], kbuf.at[j], load_sem.at[0, j]),
            pltpu.make_async_copy(value_hbm.at[:, :, cols], vbuf.at[j], load_sem.at[1, j]),
        ))
    for key_load, _ in loads:
        key_load.start()
    for _, value_load in loads:
        value_load.start()
    small[2].start()
    small[3].start()

    per = chosen.shape[1]
    small[0].wait()
    pieces = [chosen[h:h + 1, :] for h in range(kv_heads)]
    if kv_heads * per < LANES:
        pieces.append(jnp.full((1, LANES - kv_heads * per), -1, jnp.int32))
    mine = jnp.concatenate(pieces, axis=1)
    gsend[...] = mine
    gbuf[pl.ds(me, 1)] = mine[None]

    pl.semaphore_wait(barrier, n - 1)

    def g_copy(k, target, slot):
        return pltpu.make_async_remote_copy(
            src_ref=gsend, dst_ref=gbuf.at[slot], send_sem=g_send.at[k], recv_sem=g_recv.at[slot],
            device_id={"page": target}, device_id_type=pl.DeviceIdType.MESH)

    far_first(n, lambda peer: g_copy(peer, peer, me).start())

    small[1].wait()
    blank = jnp.zeros((rows, width), BF16)
    for j in range(pairs):
        parts = []
        for a in range(2):
            head = 2 * j + a
            stack = jnp.concatenate(
                [queries[:, (head * groups + g) * width:(head * groups + g + 1) * width]
                 for g in range(groups)], axis=0)
            parts.append(jnp.concatenate([stack, blank] if a == 0 else [blank, stack], axis=1))
        qbd[j] = jnp.concatenate(parts, axis=0)

    step = 4
    for j in range(pairs):
        loads[j][0].wait()
        for p in range(0, pages, step):
            keys = kbuf[j, p:p + step].reshape(step * tokens, 2 * width)
            scores = dot(keys, qbd[j], ((1,), (1,)))
            for i in range(step):
                part = scores[i * tokens:(i + 1) * tokens]
                high = jnp.ceil(jnp.max(part, axis=0, keepdims=True) * rate)
                raised = jnp.exp2(part * rate - high).astype(BF16)
                page_high[j, p + i:p + i + 1] = high
                page_sums[j, p + i:p + i + 1] = jnp.sum(raised.astype(F32), axis=0, keepdims=True)
                weights[j, p + i] = raised

    first = me * per_owner
    lanes = lax.broadcasted_iota(jnp.int32, (drafts, 2 * rows), 1)
    keys_at = lax.broadcasted_iota(jnp.int32, (drafts, 2 * rows), 0)
    small[2].wait()
    small[3].wait()
    for j in range(pairs):
        cols = slice(j * 2 * width, (j + 1) * 2 * width)
        scores = dot(new_keys[:, cols], qbd[j], ((1,), (1,)))
        head_of = lanes // drafts + j * per_pair
        ok = (keys_at <= lanes % drafts) & (head_of >= first) & (head_of < first + per_owner)
        high = jnp.ceil(jnp.max(jnp.where(ok, scores * rate, LOW), axis=0, keepdims=True))
        raised = jnp.where(ok, jnp.exp2(scores * rate - high), 0.0).astype(BF16).astype(F32)
        fresh_stats[j, 0:1] = high
        fresh_stats[j, 1:2] = jnp.sum(raised, axis=0, keepdims=True)
        fresh_weights[j] = raised

    far_first(n, lambda peer: g_copy(peer, peer, peer).wait_recv())

    page_ids = lax.broadcasted_iota(jnp.int32, (pages, LANES), 0) + me * pages
    hit = gbuf[0] == page_ids
    for source in range(1, n):
        hit = hit | (gbuf[source] == page_ids)
    lane = lax.broadcasted_iota(jnp.int32, (LANES, kv_heads * rows), 0)
    column = lax.broadcasted_iota(jnp.int32, (LANES, kv_heads * rows), 1)
    spread = jnp.where(lane // per == column // rows, 1.0, 0.0).astype(BF16)
    named = dot(jnp.where(hit, 1.0, 0.0).astype(BF16), spread, ((1,), (0,)))
    for j in range(pairs):
        picked[j] = named[:, j * 2 * rows:(j + 1) * 2 * rows]
        loads[j][1].wait()

    def o_copy(k, target, slot, owner):
        return pltpu.make_async_remote_copy(
            src_ref=obuf.at[pl.ds(owner * per_owner, per_owner)], dst_ref=orecv.at[slot],
            send_sem=o_send.at[k], recv_sem=o_recv.at[slot],
            device_id={"page": target}, device_id_type=pl.DeviceIdType.MESH)

    def s_copy(k, target, slot, owner):
        return pltpu.make_async_remote_copy(
            src_ref=sbuf.at[owner * per_owner // per_pair], dst_ref=srecv.at[slot],
            send_sem=s_send.at[k], recv_sem=s_recv.at[slot],
            device_id={"page": target}, device_id_type=pl.DeviceIdType.MESH)

    wide = 8
    plane = me * pairs // n
    for turn in range(pairs):
        back = pairs - 1 - turn
        down = back - jnp.where(back <= plane, 1, 0)
        up = turn + jnp.where(turn >= plane, 1, 0)
        j = jnp.where(me * 2 < n, down, up) if back else plane
        in_use = picked[j] > 0.5
        high_fresh = fresh_stats[j, 0:1]
        sums_fresh = fresh_stats[j, 1:2]
        highs = page_high[j]
        top = jnp.maximum(jnp.max(jnp.where(in_use, highs, LOW), axis=0, keepdims=True), high_fresh)
        share = jnp.where(in_use, jnp.exp2(highs - top), 0.0).astype(BF16)
        share_fresh = jnp.exp2(high_fresh - top)
        total = jnp.sum(share.astype(F32) * page_sums[j], axis=0, keepdims=True)
        total = total + share_fresh * sums_fresh
        acc = dot((fresh_weights[j] * share_fresh).astype(BF16),
                  new_values[:, pl.ds(pl.multiple_of(j * 2 * width, 2 * width), 2 * width)], ((0,), (0,)))
        for p in range(0, pages, wide):
            scaled = weights[j, p:p + wide] * share[p:p + wide][:, None, :]
            acc = acc + dot(scaled.reshape(wide * tokens, 2 * rows),
                            vbuf[j, p:p + wide].reshape(wide * tokens, 2 * width), ((0,), (0,)))
        sbuf[j, 0:1] = top
        sbuf[j, 1:2] = total
        for a in range(2):
            part = acc[a * rows:(a + 1) * rows, a * width:(a + 1) * width].astype(BF16)
            obuf[pl.ds((2 * j + a) * groups, groups)] = part.reshape(groups, drafts, width)

        owned = per_pair // per_owner
        for i in range(owned):
            o = j * owned + i

            @pl.when(me != o)
            def _():
                s_copy(o, o, me, o).start()
                o_copy(o, o, me, o).start()

    def block_of(owner):
        cols = per_owner * width
        return out_ref.at[:, pl.ds(pl.multiple_of(owner * cols, cols), cols)]

    def f_copy(k, target, slot):
        return pltpu.make_async_remote_copy(
            src_ref=fin, dst_ref=block_of(slot), send_sem=f_send.at[k], recv_sem=f_recv.at[slot],
            device_id={"page": target}, device_id_type=pl.DeviceIdType.MESH)

    def finish():
        srecv[pl.ds(me, 1)] = sbuf[pl.ds(me * per_owner // per_pair, 1)]
        orecv[pl.ds(me, 1)] = obuf[pl.ds(first, per_owner)][None]

        def s_wait(k, carry):
            s_copy(peer_of(k), peer_of(k), peer_of(k), me).wait_recv()
            return carry

        lax.fori_loop(1, n, s_wait, 0)
        highs = srecv[:, 0, :]
        top = jnp.max(highs, axis=0, keepdims=True)
        share = jnp.exp2(highs - top)
        total = jnp.sum(share * srecv[:, 1, :], axis=0, keepdims=True)
        factors[...] = jnp.transpose(share / total)
        own_rows = per_owner * drafts
        own = factors[pl.ds(pl.multiple_of(lax.rem(first, per_pair) * drafts, drafts), own_rows), :]

        def o_wait(k, carry):
            o_copy(peer_of(k), peer_of(k), peer_of(k), me).wait_recv()
            return carry

        lax.fori_loop(1, n, o_wait, 0)
        acc = jnp.zeros((own_rows, width), F32)
        for i in range(n):
            acc = acc + own[:, i:i + 1] * orecv[i].reshape(own_rows, width).astype(F32)
        done = acc.astype(BF16)
        for i in range(per_owner):
            fin[:, i * width:(i + 1) * width] = done[i * drafts:(i + 1) * drafts]

        far_first(n, lambda peer: f_copy(peer, peer, me).start())
        block_of(me)[...] = fin[...]

    if everyone:
        finish()
    else:
        pl.when(me < owners)(finish)

    def sent(o, carry):
        @pl.when(me != o)
        def _():
            s_copy(o, o, me, o).wait_send()
            o_copy(o, o, me, o).wait_send()
        return carry

    lax.fori_loop(0, owners, sent, 0)

    def f_wait(o, carry):
        @pl.when(me != o)
        def _():
            f_copy(o, o, o).wait_recv()
        return carry

    lax.fori_loop(0, owners, f_wait, 0)
    far_first(n, lambda peer: g_copy(peer, peer, peer).wait_send())

    def f_sent():
        far_first(n, lambda peer: f_copy(peer, peer, me).wait_send())

    if everyone:
        f_sent()
    else:
        pl.when(me < owners)(f_sent)


def on_device(queries, key_cache, value_cache, new_keys, new_values, chosen):
    n = lax.axis_size("page")
    pages, tokens, span = key_cache.shape
    drafts = queries.shape[0]
    groups = queries.shape[1] // span
    kv_heads = chosen.shape[0]
    width = span // kv_heads
    pairs = kv_heads // 2
    heads = kv_heads * groups
    rows = drafts * groups
    owners = min(n, heads)
    per_owner = heads // owners
    vmem = pl.BlockSpec(memory_space=pltpu.VMEM)
    hbm = pl.BlockSpec(memory_space=pl.ANY)
    dma = pltpu.SemaphoreType.DMA
    return pl.pallas_call(
        functools.partial(kernel, n, owners, kv_heads, groups),
        out_shape=pltpu.VMEM(queries.shape, BF16),
        in_specs=[hbm] * 6,
        out_specs=vmem,
        scratch_shapes=[
            pltpu.VMEM(queries.shape, BF16),
            pltpu.VMEM(new_keys.shape, BF16),
            pltpu.VMEM(new_values.shape, BF16),
            pltpu.VMEM(chosen.shape, jnp.int32),
            pltpu.VMEM((pairs, pages, tokens, 2 * width), BF16),
            pltpu.VMEM((pairs, pages, tokens, 2 * width), BF16),
            pltpu.VMEM((pairs, 2 * rows, 2 * width), BF16),
            pltpu.VMEM((pairs, pages, tokens, 2 * rows), BF16),
            pltpu.VMEM((pairs, pages, 2 * rows), F32),
            pltpu.VMEM((pairs, pages, 2 * rows), F32),
            pltpu.VMEM((n, 1, LANES), jnp.int32),
            pltpu.VMEM((1, LANES), jnp.int32),
            pltpu.VMEM((pairs, pages, 2 * rows), F32),
            pltpu.VMEM((pairs, 2, 2 * rows), F32),
            pltpu.VMEM((pairs, drafts, 2 * rows), F32),
            pltpu.VMEM((heads, drafts, width), BF16),
            pltpu.VMEM((pairs, 2, 2 * rows), F32),
            pltpu.VMEM((n, per_owner, drafts, width), BF16),
            pltpu.VMEM((n, 2, 2 * rows), F32),
            pltpu.VMEM((2 * rows, n), F32),
            pltpu.VMEM((drafts, per_owner * width), BF16),
            dma((4,)), dma((2, pairs)),
            dma((n,)), dma((n,)),
            dma((n,)), dma((n,)),
            dma((n,)), dma((n,)),
            dma((n,)), dma((n,)),
        ],
        compiler_params=pltpu.CompilerParams(collective_id=0, has_side_effects=True),
        name="paged_attention",
    )(queries, key_cache, value_cache, new_keys, new_values, chosen)


def solution(mesh):
    placed = (
        P("grp", None),
        P(("grp", "page"), None, None),
        P(("grp", "page"), None, None),
        P("grp", None),
        P("grp", None),
        P("grp", "page"),
    )
    return jax.shard_map(
        on_device, mesh=mesh, in_specs=placed, out_specs=P("grp", None), check_vma=False
    )
```

```python
import functools

import jax
import jax.numpy as jnp
from jax import lax
from jax.experimental import pallas as pl
from jax.experimental.pallas import tpu as pltpu
from jax.sharding import PartitionSpec as P

LOW = -1e30
LOG2E = 1.4426950408889634
LANES = 128
BF16 = jnp.bfloat16
F32 = jnp.float32


def dot(a, b, dims):
    return lax.dot_general(a, b, (dims, ((), ())), preferred_element_type=F32)


def kernel(
    n, owners, kv_heads, groups,
    queries_hbm, key_hbm, value_hbm, new_keys_hbm, new_values_hbm, chosen_hbm, out_ref,
    queries, new_keys, new_values, chosen, kbuf, vbuf, qbd, weights, page_high, page_sums, gbuf, gsend, picked, fresh_stats, fresh_weights,
    obuf, sbuf, orecv, srecv, factors, fin,
    small_sem, load_sem, g_send, g_recv, o_send, o_recv, s_send, s_recv, f_send, f_recv,
):
    me = lax.axis_index("page")
    pages, tokens, span = key_hbm.shape
    width = span // kv_heads
    drafts = queries.shape[0]
    pairs = kv_heads // 2
    rows = drafts * groups
    heads = kv_heads * groups
    per_owner = heads // owners
    per_pair = 2 * groups
    rate = width ** (-0.5) * LOG2E
    everyone = owners == n

    def peer_of(k):
        return lax.rem(me + k, n)

    def far_first(count, act):
        def body(k, carry):
            peer = jnp.where(me * 2 < n, count - 1 - k, k)
            pl.when(peer != me)(lambda: act(peer))
            return carry

        lax.fori_loop(0, count, body, 0, unroll=n <= 16)

    barrier = pltpu.get_barrier_semaphore()

    def greet(k, carry):
        pl.semaphore_signal(barrier, inc=1, device_id={"page": peer_of(k)},
                            device_id_type=pl.DeviceIdType.MESH)
        return carry

    lax.fori_loop(1, n, greet, 0, unroll=n <= 16)

    small = [
        pltpu.make_async_copy(src, dst, small_sem.at[i])
        for i, (src, dst) in enumerate((
            (chosen_hbm, chosen), (queries_hbm, queries),
            (new_keys_hbm, new_keys), (new_values_hbm, new_values)))
    ]
    small[0].start()
    small[1].start()
    loads = []
    for j in range(pairs):
        cols = pl.ds(j * 2 * width, 2 * width)
        loads.append((
            pltpu.make_async_copy(key_hbm.at[:, :, cols], kbuf.at[j], load_sem.at[0, j]),
            pltpu.make_async_copy(value_hbm.at[:, :, cols], vbuf.at[j], load_sem.at[1, j]),
        ))
    for key_load, _ in loads:
        key_load.start()
    for _, value_load in loads:
        value_load.start()
    small[2].start()
    small[3].start()

    per = chosen.shape[1]
    small[0].wait()
    pieces = [chosen[h:h + 1, :] for h in range(kv_heads)]
    if kv_heads * per < LANES:
        pieces.append(jnp.full((1, LANES - kv_heads * per), -1, jnp.int32))
    mine = jnp.concatenate(pieces, axis=1)
    gsend[...] = mine
    gbuf[pl.ds(me, 1)] = mine[None]

    pl.semaphore_wait(barrier, n - 1)

    def g_copy(k, target, slot):
        return pltpu.make_async_remote_copy(
            src_ref=gsend, dst_ref=gbuf.at[slot], send_sem=g_send.at[k], recv_sem=g_recv.at[slot],
            device_id={"page": target}, device_id_type=pl.DeviceIdType.MESH)

    far_first(n, lambda peer: g_copy(peer, peer, me).start())

    small[1].wait()
    blank = jnp.zeros((rows, width), BF16)
    for j in range(pairs):
        parts = []
        for a in range(2):
            head = 2 * j + a
            stack = jnp.concatenate(
                [queries[:, (head * groups + g) * width:(head * groups + g + 1) * width]
                 for g in range(groups)], axis=0)
            parts.append(jnp.concatenate([stack, blank] if a == 0 else [blank, stack], axis=1))
        qbd[j] = jnp.concatenate(parts, axis=0)

    step = 4
    for j in range(pairs):
        loads[j][0].wait()
        for p in range(0, pages, step):
            keys = kbuf[j, p:p + step].reshape(step * tokens, 2 * width)
            scores = dot(keys, qbd[j], ((1,), (1,)))
            for i in range(step):
                part = scores[i * tokens:(i + 1) * tokens]
                high = jnp.ceil(jnp.max(part, axis=0, keepdims=True) * rate)
                raised = jnp.exp2(part * rate - high).astype(BF16)
                page_high[j, p + i:p + i + 1] = high
                page_sums[j, p + i:p + i + 1] = jnp.sum(raised.astype(F32), axis=0, keepdims=True)
                weights[j, p + i] = raised

    first = me * per_owner
    lanes = lax.broadcasted_iota(jnp.int32, (drafts, 2 * rows), 1)
    keys_at = lax.broadcasted_iota(jnp.int32, (drafts, 2 * rows), 0)
    small[2].wait()
    small[3].wait()
    for j in range(pairs):
        cols = slice(j * 2 * width, (j + 1) * 2 * width)
        scores = dot(new_keys[:, cols], qbd[j], ((1,), (1,)))
        head_of = lanes // drafts + j * per_pair
        ok = (keys_at <= lanes % drafts) & (head_of >= first) & (head_of < first + per_owner)
        high = jnp.ceil(jnp.max(jnp.where(ok, scores * rate, LOW), axis=0, keepdims=True))
        raised = jnp.where(ok, jnp.exp2(scores * rate - high), 0.0).astype(BF16).astype(F32)
        fresh_stats[j, 0:1] = high
        fresh_stats[j, 1:2] = jnp.sum(raised, axis=0, keepdims=True)
        fresh_weights[j] = raised

    far_first(n, lambda peer: g_copy(peer, peer, peer).wait_recv())

    page_ids = lax.broadcasted_iota(jnp.int32, (pages, LANES), 0) + me * pages
    hit = gbuf[0] == page_ids
    for source in range(1, n):
        hit = hit | (gbuf[source] == page_ids)
    lane = lax.broadcasted_iota(jnp.int32, (LANES, kv_heads * rows), 0)
    column = lax.broadcasted_iota(jnp.int32, (LANES, kv_heads * rows), 1)
    spread = jnp.where(lane // per == column // rows, 1.0, 0.0).astype(BF16)
    named = dot(jnp.where(hit, 1.0, 0.0).astype(BF16), spread, ((1,), (0,)))
    for j in range(pairs):
        picked[j] = named[:, j * 2 * rows:(j + 1) * 2 * rows]
        loads[j][1].wait()

    def o_copy(k, target, slot, owner):
        return pltpu.make_async_remote_copy(
            src_ref=obuf.at[pl.ds(owner * per_owner, per_owner)], dst_ref=orecv.at[slot],
            send_sem=o_send.at[k], recv_sem=o_recv.at[slot],
            device_id={"page": target}, device_id_type=pl.DeviceIdType.MESH)

    def s_copy(k, target, slot, owner):
        return pltpu.make_async_remote_copy(
            src_ref=sbuf.at[owner * per_owner // per_pair], dst_ref=srecv.at[slot],
            send_sem=s_send.at[k], recv_sem=s_recv.at[slot],
            device_id={"page": target}, device_id_type=pl.DeviceIdType.MESH)

    wide = 8
    plane = me * pairs // n
    for turn in range(pairs):
        back = pairs - 1 - turn
        down = back - jnp.where(back <= plane, 1, 0)
        up = turn + jnp.where(turn >= plane, 1, 0)
        j = jnp.where(me * 2 < n, down, up) if back else plane
        in_use = picked[j] > 0.5
        high_fresh = fresh_stats[j, 0:1]
        sums_fresh = fresh_stats[j, 1:2]
        highs = page_high[j]
        top = jnp.maximum(jnp.max(jnp.where(in_use, highs, LOW), axis=0, keepdims=True), high_fresh)
        share = jnp.where(in_use, jnp.exp2(highs - top), 0.0).astype(BF16)
        share_fresh = jnp.exp2(high_fresh - top)
        total = jnp.sum(share.astype(F32) * page_sums[j], axis=0, keepdims=True)
        total = total + share_fresh * sums_fresh
        acc = dot((fresh_weights[j] * share_fresh).astype(BF16),
                  new_values[:, pl.ds(pl.multiple_of(j * 2 * width, 2 * width), 2 * width)], ((0,), (0,)))
        for p in range(0, pages, wide):
            scaled = weights[j, p:p + wide] * share[p:p + wide][:, None, :]
            acc = acc + dot(scaled.reshape(wide * tokens, 2 * rows),
                            vbuf[j, p:p + wide].reshape(wide * tokens, 2 * width), ((0,), (0,)))
        sbuf[j, 0:1] = top
        sbuf[j, 1:2] = total
        for a in range(2):
            part = acc[a * rows:(a + 1) * rows, a * width:(a + 1) * width].astype(BF16)
            obuf[pl.ds((2 * j + a) * groups, groups)] = part.reshape(groups, drafts, width)

        owned = per_pair // per_owner
        for i in range(owned):
            o = j * owned + i

            @pl.when(me != o)
            def _():
                s_copy(o, o, me, o).start()
                o_copy(o, o, me, o).start()

    def block_of(owner):
        cols = per_owner * width
        return out_ref.at[:, pl.ds(pl.multiple_of(owner * cols, cols), cols)]

    def f_copy(k, target, slot):
        return pltpu.make_async_remote_copy(
            src_ref=fin, dst_ref=block_of(slot), send_sem=f_send.at[k], recv_sem=f_recv.at[slot],
            device_id={"page": target}, device_id_type=pl.DeviceIdType.MESH)

    def finish():
        srecv[pl.ds(me, 1)] = sbuf[pl.ds(me * per_owner // per_pair, 1)]
        orecv[pl.ds(me, 1)] = obuf[pl.ds(first, per_owner)][None]

        def s_wait(k, carry):
            s_copy(peer_of(k), peer_of(k), peer_of(k), me).wait_recv()
            return carry

        lax.fori_loop(1, n, s_wait, 0, unroll=n <= 16)
        highs = srecv[:, 0, :]
        top = jnp.max(highs, axis=0, keepdims=True)
        share = jnp.exp2(highs - top)
        total = jnp.sum(share * srecv[:, 1, :], axis=0, keepdims=True)
        factors[...] = jnp.transpose(share / total)
        own_rows = per_owner * drafts
        own = factors[pl.ds(pl.multiple_of(lax.rem(first, per_pair) * drafts, drafts), own_rows), :]

        def o_wait(k, carry):
            o_copy(peer_of(k), peer_of(k), peer_of(k), me).wait_recv()
            return carry

        lax.fori_loop(1, n, o_wait, 0, unroll=n <= 16)
        acc = jnp.zeros((own_rows, width), F32)
        for i in range(n):
            acc = acc + own[:, i:i + 1] * orecv[i].reshape(own_rows, width).astype(F32)
        done = acc.astype(BF16)
        for i in range(per_owner):
            fin[:, i * width:(i + 1) * width] = done[i * drafts:(i + 1) * drafts]

        far_first(n, lambda peer: f_copy(peer, peer, me).start())
        block_of(me)[...] = fin[...]

    if everyone:
        finish()
    else:
        pl.when(me < owners)(finish)

    def sent(o, carry):
        @pl.when(me != o)
        def _():
            s_copy(o, o, me, o).wait_send()
            o_copy(o, o, me, o).wait_send()
        return carry

    lax.fori_loop(0, owners, sent, 0, unroll=n <= 16)

    def f_wait(o, carry):
        @pl.when(me != o)
        def _():
            f_copy(o, o, o).wait_recv()
        return carry

    lax.fori_loop(0, owners, f_wait, 0, unroll=n <= 16)
    far_first(n, lambda peer: g_copy(peer, peer, peer).wait_send())

    def f_sent():
        far_first(n, lambda peer: f_copy(peer, peer, me).wait_send())

    if everyone:
        f_sent()
    else:
        pl.when(me < owners)(f_sent)


def on_device(queries, key_cache, value_cache, new_keys, new_values, chosen):
    n = lax.axis_size("page")
    pages, tokens, span = key_cache.shape
    drafts = queries.shape[0]
    groups = queries.shape[1] // span
    kv_heads = chosen.shape[0]
    width = span // kv_heads
    pairs = kv_heads // 2
    heads = kv_heads * groups
    rows = drafts * groups
    owners = min(n, heads)
    per_owner = heads // owners
    vmem = pl.BlockSpec(memory_space=pltpu.VMEM)
    hbm = pl.BlockSpec(memory_space=pl.ANY)
    dma = pltpu.SemaphoreType.DMA
    return pl.pallas_call(
        functools.partial(kernel, n, owners, kv_heads, groups),
        out_shape=pltpu.VMEM(queries.shape, BF16),
        in_specs=[hbm] * 6,
        out_specs=vmem,
        scratch_shapes=[
            pltpu.VMEM(queries.shape, BF16),
            pltpu.VMEM(new_keys.shape, BF16),
            pltpu.VMEM(new_values.shape, BF16),
            pltpu.VMEM(chosen.shape, jnp.int32),
            pltpu.VMEM((pairs, pages, tokens, 2 * width), BF16),
            pltpu.VMEM((pairs, pages, tokens, 2 * width), BF16),
            pltpu.VMEM((pairs, 2 * rows, 2 * width), BF16),
            pltpu.VMEM((pairs, pages, tokens, 2 * rows), BF16),
            pltpu.VMEM((pairs, pages, 2 * rows), F32),
            pltpu.VMEM((pairs, pages, 2 * rows), F32),
            pltpu.VMEM((n, 1, LANES), jnp.int32),
            pltpu.VMEM((1, LANES), jnp.int32),
            pltpu.VMEM((pairs, pages, 2 * rows), F32),
            pltpu.VMEM((pairs, 2, 2 * rows), F32),
            pltpu.VMEM((pairs, drafts, 2 * rows), F32),
            pltpu.VMEM((heads, drafts, width), BF16),
            pltpu.VMEM((pairs, 2, 2 * rows), F32),
            pltpu.VMEM((n, per_owner, drafts, width), BF16),
            pltpu.VMEM((n, 2, 2 * rows), F32),
            pltpu.VMEM((2 * rows, n), F32),
            pltpu.VMEM((drafts, per_owner * width), BF16),
            dma((4,)), dma((2, pairs)),
            dma((n,)), dma((n,)),
            dma((n,)), dma((n,)),
            dma((n,)), dma((n,)),
            dma((n,)), dma((n,)),
        ],
        compiler_params=pltpu.CompilerParams(collective_id=0, has_side_effects=True),
        name="paged_attention",
    )(queries, key_cache, value_cache, new_keys, new_values, chosen)


def solution(mesh):
    placed = (
        P("grp", None),
        P(("grp", "page"), None, None),
        P(("grp", "page"), None, None),
        P("grp", None),
        P("grp", None),
        P("grp", "page"),
    )
    return jax.shard_map(
        on_device, mesh=mesh, in_specs=placed, out_specs=P("grp", None), check_vma=False
    )
```
